32 devices in a mesh: member: 2 (over x), region: 16 (over z, y, core).
Axes of the slice: x: 2, y: 2, z: 4, core: 2. Of those that a mesh axis runs over, the one named last changes fastest.
Arguments:
- mesh_nodes: bfloat16 [16384, 512], P(('member', 'region')), parts along dimension 0, may hold values from -6 to 6
- mesh_edges: bfloat16 [32768, 512], P('region'), may hold values from -6 to 6
- grid_nodes: bfloat16 [12288, 512], P(('member', 'region')), parts along dimension 0, may hold values from -6 to 6
- grid_edges: bfloat16 [18432, 512], P('region'), may hold values from -6 to 6
- boundary: int32 [16, 32], P('region'), may hold values from 0 to 511
- mesh_need: int32 [16, 16, 8], P('region'), may hold values from 0 to 31
- mesh_sender: int32 [16, 2048], P('region'), may hold values from 0 to 639, as said below
- mesh_receiver: int32 [16, 2048], P('region'), may hold values from 0 to 511
- mesh_live: int32 [16], P('region'), may hold values from 512 to 2048, as said below
- grid_need: int32 [16, 4, 8], P('region'), may hold values from 0 to 31
- grid_sender: int32 [16, 1152], P('region'), may hold values from 0 to 543, as said below
- grid_receiver: int32 [16, 1152], P('region'), may hold values from 0 to 383
- process_edge_in: bfloat16 [1536, 512], replicated, may hold values from -0.15625 to 0.15625
- process_edge_bias: float32 [512], replicated, may hold values from -3 to 3
- process_edge_out: bfloat16 [512, 512], replicated, may hold values from -0.25 to 0.25
- process_edge_gain: float32 [512], replicated, may hold values from 0.5 to 1.5
- process_node_in: bfloat16 [1024, 512], replicated, may hold values from -0.1875 to 0.1875
- process_node_bias: float32 [512], replicated, may hold values from -3 to 3
- process_node_out: bfloat16 [512, 512], replicated, may hold values from -0.25 to 0.25
- process_node_gain: float32 [512], replicated, may hold values from 0.5 to 1.5
- decode_edge_in: bfloat16 [1536, 512], replicated, may hold values from -0.15625 to 0.15625
- decode_edge_bias: float32 [512], replicated, may hold values from -3 to 3
- decode_edge_out: bfloat16 [512, 512], replicated, may hold values from -0.25 to 0.25
- decode_edge_gain: float32 [512], replicated, may hold values from 0.5 to 1.5
- decode_node_in: bfloat16 [1024, 512], replicated, may hold values from -0.1875 to 0.1875
- decode_node_bias: float32 [512], replicated, may hold values from -3 to 3
- decode_node_out: bfloat16 [512, 512], replicated, may hold values from -0.25 to 0.25
- decode_node_gain: float32 [512], replicated, may hold values from 0.5 to 1.5
Outputs:
- mesh_out: bfloat16 [16384, 512], P(('member', 'region')), parts along dimension 0
- grid_out: bfloat16 [12288, 512], P(('member', 'region')), parts along dimension 0
The draws below stay inside these ranges and needn't reach their ends.
There are 2 independent parts, one for each index of `member`. The reference program is written for one: setup_inputs(seed, part) draws one part's arguments, and reference() takes and returns one part's arrays. A program takes and returns all parts, laid end to end along the dimension named above; an argument that names none is the same for every part. Nothing has to cross between parts.
Inputs may be any that keep to these rules, and one draw needn't show every extreme that they name: The first mesh_live[d] slots of region d are live and the rest are padding; in every draw some region has all 2048 slots live. `mesh_sender`: a value below 512 names a node of the region itself; 512 + s * 8 + k names the k-th node that the region reads from region s; most slots name the region's own nodes, most remote reads come from its four neighbours, and a few reach any region. `grid_sender`: a value below 512 names a node of the region's mesh_out; 512 + j * 8 + k names the k-th node read from its j-th neighbour; most edges name the region's own nodes.
All inputs are finite; a program needn't handle non-finite values.
Results may differ from the reference program's by a relative error of at most 0.007.
Values may be sent and summed in bfloat16 or wider, within the bound.
A program may use at most 64 MiB of HBM per device.

```python
import jax
import jax.numpy as jnp
from jax import lax

LATENT = 512
MESH_DEV = 512
GRID_DEV = 384
BOUNDARY = 32
PAIR = 8
REGIONS = 16
EDGES = 2048
GRID_EDGES = 1152
MESH_NODES = 8192
GRID_NODES = 6144


def draw_mesh_live(key, part):
    first_key, second_key = jax.random.split(jax.random.fold_in(key, 11))
    counts = jax.random.randint(first_key, (REGIONS,), EDGES // 4, EDGES + 1)
    fullest = jax.random.randint(second_key, (), 0, REGIONS)
    return jnp.where(jnp.arange(REGIONS) == fullest, EDGES, counts).astype(jnp.int32)


def draw_mesh_sender(key, part):
    keys = jax.random.split(jax.random.fold_in(key, 23), 5)
    shape = (REGIONS, EDGES)
    kind = jax.random.randint(keys[0], shape, 0, 10)
    local = jax.random.randint(keys[1], shape, 0, MESH_DEV)
    offsets = jnp.array([-2, -1, 1, 2], dtype=jnp.int32)
    near = offsets[jax.random.randint(keys[2], shape, 0, 4)]
    region = jnp.arange(REGIONS, dtype=jnp.int32)[:, None]
    near_source = (region + near) % REGIONS
    far_source = jax.random.randint(keys[3], shape, 0, REGIONS)
    slot = jax.random.randint(keys[4], shape, 0, PAIR)
    source = jnp.where(kind < 9, near_source, far_source)
    remote = MESH_DEV + source * PAIR + slot
    return jnp.where(kind < 6, local, remote).astype(jnp.int32)


def draw_grid_sender(key, part):
    keys = jax.random.split(jax.random.fold_in(key, 37), 3)
    shape = (REGIONS, GRID_EDGES)
    kind = jax.random.randint(keys[0], shape, 0, 5)
    local = jax.random.randint(keys[1], shape, 0, MESH_DEV)
    remote = MESH_DEV + jax.random.randint(keys[2], shape, 0, 4 * PAIR)
    return jnp.where(kind < 4, local, remote).astype(jnp.int32)


def place_ends(result, rng, smallest, top_value):
    longest = result.shape.index(max(result.shape))
    spots = []
    for shift in (0, 1):
        where = [jax.random.randint(jax.random.fold_in(rng, axis), (), 0, length) for axis, length in enumerate(result.shape)]
        where[longest] = (where[longest] + shift) % result.shape[longest]
        spots.append(tuple(where))
    return result.at[spots[0]].set(smallest).at[spots[1]].set(top_value)


def shard_levels(key, shape, shards, low, top_value):
    def one(axis_at, shards_of):
        heights = jax.random.uniform(jax.random.fold_in(jax.random.fold_in(key, 6), axis_at), (shards_of,), jnp.float32, low / len(shards), top_value / len(shards))
        return jnp.repeat(jnp.exp(heights), shape[axis_at] // shards_of).reshape((-1,) + (1,) * (len(shape) - axis_at - 1))

    level = one(*shards[0])
    for cut in shards[1:]:
        level = level * one(*cut)
    return level


def gaussian(rng, extent, deviation, most, cuts=(), held_as=jnp.bfloat16):
    values = deviation * jax.random.normal(rng, extent, jnp.float32)
    if cuts:
        values = values * shard_levels(rng, extent, cuts, -0.22, 0.18)
    return jnp.clip(values, -most, most).astype(held_as)


def setup_inputs(seed: int = 0, part: int = 0) -> dict:
    key_list = jax.random.split(jax.random.key(seed), 29)
    own_keys = jax.random.split(jax.random.fold_in(key_list[28], part), 29)
    mesh_nodes = gaussian(own_keys[0], (MESH_NODES, LATENT), 1.0, 6.0, ((0, 16),))
    mesh_edges = gaussian(key_list[1], (REGIONS * EDGES, LATENT), 1.0, 6.0, ((0, 16),))
    grid_nodes = gaussian(own_keys[2], (GRID_NODES, LATENT), 1.0, 6.0, ((0, 16),))
    grid_edges = gaussian(key_list[3], (REGIONS * GRID_EDGES, LATENT), 1.0, 6.0, ((0, 16),))
    boundary = place_ends(jax.random.randint(key_list[4], (REGIONS, BOUNDARY), 0, MESH_DEV), jax.random.fold_in(key_list[4], 1), 0, MESH_DEV - 1).astype(jnp.int32)
    mesh_need = place_ends(jax.random.randint(key_list[5], (REGIONS, REGIONS, PAIR), 0, BOUNDARY), jax.random.fold_in(key_list[5], 1), 0, BOUNDARY - 1).astype(jnp.int32)
    mesh_sender = draw_mesh_sender(jax.random.fold_in(key_list[28], 71), part)
    mesh_receiver = place_ends(jax.random.randint(key_list[7], (REGIONS, EDGES), 0, MESH_DEV), jax.random.fold_in(key_list[7], 1), 0, MESH_DEV - 1).astype(jnp.int32)
    mesh_live = draw_mesh_live(jax.random.fold_in(key_list[28], 71), part)
    grid_need = place_ends(jax.random.randint(key_list[9], (REGIONS, 4, PAIR), 0, BOUNDARY), jax.random.fold_in(key_list[9], 1), 0, BOUNDARY - 1).astype(jnp.int32)
    grid_sender = draw_grid_sender(jax.random.fold_in(key_list[28], 71), part)
    grid_receiver = place_ends(jax.random.randint(key_list[11], (REGIONS, GRID_EDGES), 0, GRID_DEV), jax.random.fold_in(key_list[11], 1), 0, GRID_DEV - 1).astype(jnp.int32)
    process_edge_in = gaussian(key_list[12], (3 * LATENT, LATENT), (3 * LATENT) ** -0.5, 0.15625)
    process_edge_bias = gaussian(key_list[13], (LATENT,), 0.5, 3.0, (), jnp.float32)
    process_edge_out = gaussian(key_list[14], (LATENT, LATENT), LATENT ** -0.5, 0.25)
    process_edge_gain = jnp.clip(1.0 + 0.1 * jax.random.normal(key_list[15], (LATENT,), jnp.float32), 0.5, 1.5)
    process_node_in = gaussian(key_list[16], (2 * LATENT, LATENT), (2 * LATENT) ** -0.5, 0.1875)
    process_node_bias = gaussian(key_list[17], (LATENT,), 0.5, 3.0, (), jnp.float32)
    process_node_out = gaussian(key_list[18], (LATENT, LATENT), LATENT ** -0.5, 0.25)
    process_node_gain = jnp.clip(1.0 + 0.1 * jax.random.normal(key_list[19], (LATENT,), jnp.float32), 0.5, 1.5)
    decode_edge_in = gaussian(key_list[20], (3 * LATENT, LATENT), (3 * LATENT) ** -0.5, 0.15625)
    decode_edge_bias = gaussian(key_list[21], (LATENT,), 0.5, 3.0, (), jnp.float32)
    decode_edge_out = gaussian(key_list[22], (LATENT, LATENT), LATENT ** -0.5, 0.25)
    decode_edge_gain = jnp.clip(1.0 + 0.1 * jax.random.normal(key_list[23], (LATENT,), jnp.float32), 0.5, 1.5)
    decode_node_in = gaussian(key_list[24], (2 * LATENT, LATENT), (2 * LATENT) ** -0.5, 0.1875)
    decode_node_bias = gaussian(key_list[25], (LATENT,), 0.5, 3.0, (), jnp.float32)
    decode_node_out = gaussian(key_list[26], (LATENT, LATENT), LATENT ** -0.5, 0.25)
    decode_node_gain = jnp.clip(1.0 + 0.1 * jax.random.normal(key_list[27], (LATENT,), jnp.float32), 0.5, 1.5)
    return dict(mesh_nodes=mesh_nodes, mesh_edges=mesh_edges, grid_nodes=grid_nodes, grid_edges=grid_edges, boundary=boundary, mesh_need=mesh_need, mesh_sender=mesh_sender, mesh_receiver=mesh_receiver, mesh_live=mesh_live, grid_need=grid_need, grid_sender=grid_sender, grid_receiver=grid_receiver, process_edge_in=process_edge_in, process_edge_bias=process_edge_bias, process_edge_out=process_edge_out, process_edge_gain=process_edge_gain, process_node_in=process_node_in, process_node_bias=process_node_bias, process_node_out=process_node_out, process_node_gain=process_node_gain, decode_edge_in=decode_edge_in, decode_edge_bias=decode_edge_bias, decode_edge_out=decode_edge_out, decode_edge_gain=decode_edge_gain, decode_node_in=decode_node_in, decode_node_bias=decode_node_bias, decode_node_out=decode_node_out, decode_node_gain=decode_node_gain)


def network(inputs, w_in, bias, w_out, gain):
    pre_act = jnp.dot(inputs, w_in, preferred_element_type=jnp.float32) + bias
    hidden = jax.nn.silu(pre_act).astype(jnp.bfloat16)
    projected = jnp.dot(hidden, w_out, preferred_element_type=jnp.float32)
    centred = projected - lax.optimization_barrier(jnp.mean(projected, axis=-1, keepdims=True))
    spread = lax.optimization_barrier(jnp.mean(centred * centred, axis=-1, keepdims=True))
    return centred * lax.rsqrt(spread + 0.25) * gain

def halo_for(node_blocks, boundary, need, region):
    chosen = jnp.take_along_axis(boundary, need[region], axis=1)
    remote = node_blocks[jnp.arange(REGIONS, dtype=jnp.int32)[:, None], chosen]
    return jnp.concatenate([node_blocks[region], remote.reshape(-1, LATENT)], axis=0)

def neighbour_halo(node_blocks, boundary, need, region):
    pieces = [node_blocks[region]]
    for slot, offset in enumerate((-2, -1, 1, 2)):
        source = ((region + offset) % REGIONS).astype(jnp.int32)
        chosen = boundary[source][need[region, slot]]
        pieces.append(node_blocks[source][chosen])
    return jnp.concatenate(pieces, axis=0)

def reference(mesh_nodes, mesh_edges, grid_nodes, grid_edges, boundary, mesh_need, mesh_sender, mesh_receiver, mesh_live, grid_need, grid_sender, grid_receiver, process_edge_in, process_edge_bias, process_edge_out, process_edge_gain, process_node_in, process_node_bias, process_node_out, process_node_gain, decode_edge_in, decode_edge_bias, decode_edge_out, decode_edge_gain, decode_node_in, decode_node_bias, decode_node_out, decode_node_gain):
    mesh_blocks = mesh_nodes.reshape(REGIONS, MESH_DEV, LATENT)
    edge_blocks = mesh_edges.reshape(REGIONS, EDGES, LATENT)
    grid_blocks = grid_nodes.reshape(REGIONS, GRID_DEV, LATENT)
    grid_edge_blocks = grid_edges.reshape(REGIONS, GRID_EDGES, LATENT)

    def mesh_region(region):
        halo_rows = halo_for(mesh_blocks, boundary, mesh_need, region)
        own_rows = mesh_blocks[region]
        edge_rows = edge_blocks[region]
        inputs = jnp.concatenate([halo_rows[mesh_sender[region]], own_rows[mesh_receiver[region]], edge_rows], axis=1)
        message = edge_rows.astype(jnp.float32) + network(inputs, process_edge_in, process_edge_bias, process_edge_out, process_edge_gain)
        live_slots = jnp.arange(EDGES, dtype=jnp.int32) < mesh_live[region]
        message = jnp.where(live_slots[:, None], message, 0.0).astype(jnp.bfloat16)
        summed = jax.ops.segment_sum(message.astype(jnp.float32), mesh_receiver[region], num_segments=MESH_DEV).astype(jnp.bfloat16)
        update = network(jnp.concatenate([own_rows, summed], axis=1), process_node_in, process_node_bias, process_node_out, process_node_gain)
        return (own_rows.astype(jnp.float32) + update).astype(jnp.bfloat16)
    mesh_out_blocks = lax.map(mesh_region, jnp.arange(REGIONS, dtype=jnp.int32))

    def grid_region(region):
        halo_rows = neighbour_halo(mesh_out_blocks, boundary, grid_need, region)
        own_rows = grid_blocks[region]
        edge_rows = grid_edge_blocks[region]
        inputs = jnp.concatenate([halo_rows[grid_sender[region]], own_rows[grid_receiver[region]], edge_rows], axis=1)
        message = (edge_rows.astype(jnp.float32) + network(inputs, decode_edge_in, decode_edge_bias, decode_edge_out, decode_edge_gain)).astype(jnp.bfloat16)
        summed = jax.ops.segment_sum(message.astype(jnp.float32), grid_receiver[region], num_segments=GRID_DEV).astype(jnp.bfloat16)
        update = network(jnp.concatenate([own_rows, summed], axis=1), decode_node_in, decode_node_bias, decode_node_out, decode_node_gain)
        return (own_rows.astype(jnp.float32) + update).astype(jnp.bfloat16)
    grid_out_blocks = lax.map(grid_region, jnp.arange(REGIONS, dtype=jnp.int32))
    return (mesh_out_blocks.reshape(-1, LATENT), grid_out_blocks.reshape(-1, LATENT))
```

```python
import functools

import jax
import jax.numpy as jnp
from jax import lax
from jax.experimental import pallas as pl
from jax.experimental.pallas import tpu as pltpu
from jax.sharding import PartitionSpec as P

F32 = jnp.float32
BF16 = jnp.bfloat16
I32 = jnp.int32
OFFSETS = (-2, -1, 1, 2)
LANES = 128
SUB = 8
BLOCK = 512
GRID_BLOCK = 384


def dot(a, b):
    return jnp.dot(a, b, preferred_element_type=F32)


def silu(x):
    half = 0.5 * x
    return half * jnp.tanh(half) + half


def normed(hidden, w_out, gain):
    projected = dot(hidden, w_out)
    centred = projected - jnp.mean(projected, axis=-1, keepdims=True)
    spread = jnp.mean(centred * centred, axis=-1, keepdims=True)
    return centred * lax.rsqrt(spread + 0.25) * gain


def lane_hot(column, first, count):
    lane = lax.broadcasted_iota(I32, column.shape, 1) + first
    pieces = [
        jnp.where(column == lane + start, 1.0, 0.0).astype(BF16) for start in range(0, count, LANES)
    ]
    return pieces[0] if len(pieces) == 1 else jnp.concatenate(pieces, axis=1)


def row_hot(row, count):
    place = lax.broadcasted_iota(I32, (count, row.shape[1]), 0)
    return jnp.where(place == row, 1.0, 0.0).astype(BF16)


def column_of(scalars):
    sub = lax.broadcasted_iota(I32, (SUB, LANES), 0)
    pieces = []
    for start in range(0, len(scalars), SUB):
        piece = jnp.full((SUB, LANES), scalars[start], I32)
        for k in range(1, SUB):
            piece = jnp.where(sub == k, scalars[start + k], piece)
        pieces.append(piece)
    return pieces[0] if len(pieces) == 1 else jnp.concatenate(pieces, axis=0)


def up(count, unit=LANES):
    return -(-count // unit) * unit


def kernel(
    sizes,
    live_hbm,
    boundary_hbm,
    need_hbm,
    gneed_hbm,
    mesh_nodes_hbm,
    mesh_edges_hbm,
    grid_nodes_hbm,
    grid_edges_hbm,
    mesh_sender_hbm,
    mesh_receiver_hbm,
    grid_sender_hbm,
    grid_receiver_hbm,
    pe_in, pe_b, pe_out, pe_g,
    pn_in, pn_b, pn_out, pn_g,
    de_in, de_b, de_out, de_g,
    dn_in, dn_b, dn_out, dn_g,
    mesh_out_ref,
    grid_out_ref,
    live, offers, need, gneed, senders, receivers, gsenders, greceivers,
    own, edges, gnodes, gedges, recv_row, grecv_row,
    w_pe, w_po, w_pn, w_pno, w_de, w_do, w_dn, w_dno, vec,
    tab_s, tab_r, gtab_s, gtab_r, picked, gpicked,
    pre, gpre, npre, gnpre, total, gtotal, updated,
    pub, everyone, pub_out, arrived, mesh_stage, grid_stage,
    write_sem, load_sem, send_sem, recv_sem, pass_send_sem, pass_recv_sem, out_send_sem, out_recv_sem,
):
    regions, offer, pair, n, m, edge_count, g, gedge_count = sizes
    slots, gslots = regions * pair, len(OFFSETS) * pair
    chunks = m // LANES
    me = lax.axis_index("region")

    loads = {}

    def load(name, source, target):
        copy = pltpu.make_async_copy(source, target, load_sem.at[len(loads)])
        copy.start()
        loads[name] = copy

    load("offers", boundary_hbm, offers)
    load("own", mesh_nodes_hbm, own)

    barrier = pltpu.get_barrier_semaphore()

    def greet(step, carry):
        pl.semaphore_signal(
            barrier,
            inc=1,
            device_id={"region": lax.rem(me + step, regions)},
            device_id_type=pl.DeviceIdType.MESH,
        )
        return carry

    lax.fori_loop(1, regions, greet, 0)

    load("w_s", pe_in.at[pl.ds(0, m)], w_pe.at[pl.ds(0, m)])
    load("w_r", pe_in.at[pl.ds(m, m)], w_pe.at[pl.ds(m, m)])
    for at, one in enumerate((pe_b, pe_g, pn_b, pn_g, de_b, de_g, dn_b, dn_g)):
        load(("vec", at), one, vec.at[at])
    load("receivers", mesh_receiver_hbm, receivers)
    load("senders", mesh_sender_hbm, senders)
    load("greceivers", grid_receiver_hbm, greceivers)
    load("gsenders", grid_sender_hbm, gsenders)
    load("need", need_hbm, need)
    load("gneed", gneed_hbm, gneed)
    load("live", live_hbm, live)
    load("w_e", pe_in.at[pl.ds(2 * m, m)], w_pe.at[pl.ds(2 * m, m)])
    for start in range(0, edge_count, BLOCK):
        load(("edges", start), mesh_edges_hbm.at[pl.ds(start, BLOCK)], edges.at[pl.ds(start, BLOCK)])
    load("w_pn", pn_in, w_pn)
    load("gnodes", grid_nodes_hbm, gnodes)
    load("w_de", de_in, w_de)
    load("gedges", grid_edges_hbm, gedges)
    load("w_dn", dn_in, w_dn)
    load("recv_row", mesh_receiver_hbm, recv_row)
    load("grecv_row", grid_receiver_hbm, grecv_row)
    load("w_po", pe_out, w_po)
    load("w_pno", pn_out, w_pno)
    load("w_do", de_out, w_do)
    load("w_dno", dn_out, w_dno)

    loads["offers"].wait()
    offer_col = column_of([offers[0, k] for k in range(offer)])
    offer_hot = lane_hot(offer_col, 0, n)
    loads["own"].wait()
    pub[...] = dot(offer_hot, own[...]).astype(BF16)
    pl.semaphore_wait(barrier, regions - 1)

    half = regions // 2
    partner = me + 1 - 2 * lax.rem(me, 2)

    def block_of(region):
        return everyone.at[pl.ds(pl.multiple_of(region * offer, offer), offer)]

    def send(step, carry):
        pltpu.make_async_remote_copy(
            src_ref=pub,
            dst_ref=block_of(me),
            send_sem=send_sem,
            recv_sem=recv_sem,
            device_id={"region": lax.rem(me + 2 * step, regions)},
            device_id_type=pl.DeviceIdType.MESH,
        ).start()
        return carry

    def to_partner(source, region):
        pltpu.make_async_remote_copy(
            src_ref=source,
            dst_ref=block_of(region),
            send_sem=pass_send_sem,
            recv_sem=pass_recv_sem,
            device_id={"region": partner},
            device_id_type=pl.DeviceIdType.MESH,
        ).start()

    lax.fori_loop(1, half, send, 0)
    to_partner(pub, me)
    everyone[pl.ds(pl.multiple_of(me * offer, offer), offer), :] = pub[...]

    def scatter_rows(target, first, rows, values):
        for c in range(chunks):
            target[pl.ds(first * chunks + c, rows, stride=chunks), :] = values[:, c * LANES : (c + 1) * LANES]

    def gathered_rows(source, first, rows):
        return jnp.concatenate(
            [source[pl.ds(first * chunks + c, rows, stride=chunks), :] for c in range(chunks)], axis=1
        )

    def pick(target, table, index, first, count):
        def one(at, carry):
            row = index[0, first + at]
            target[pl.ds(at * chunks, chunks), :] = table[pl.ds(row * chunks, chunks), :]
            return carry

        lax.fori_loop(0, count, one, 0, unroll=True)

    for at in range(8):
        loads[("vec", at)].wait()
    loads["w_r"].wait()
    scatter_rows(tab_r, 0, n, dot(own[...], w_pe[pl.ds(m, m), :]) + vec[0])
    loads["w_s"].wait()
    scatter_rows(tab_s, 0, n, dot(own[...], w_pe[pl.ds(0, m), :]))
    for name in ("receivers", "senders", "greceivers", "gsenders", "need", "gneed", "live"):
        loads[name].wait()
    need_col = column_of([need[k, s] + s * offer for s in range(regions) for k in range(pair)])
    gneed_col = column_of([gneed[j, k] + j * offer for j in range(len(OFFSETS)) for k in range(pair)])
    loads["w_e"].wait()
    for start in range(0, edge_count, BLOCK):
        loads[("edges", start)].wait()
    for start in range(0, edge_count, BLOCK):
        rows = pl.ds(start, BLOCK)
        pick(picked.at[start // BLOCK % 2], tab_r, receivers, start, BLOCK)
        pre[rows, :] = dot(edges[rows, :], w_pe[pl.ds(2 * m, m), :]) + gathered_rows(
            picked.at[start // BLOCK % 2], 0, BLOCK
        )

    for name in ("w_pn", "gnodes", "w_de", "gedges", "w_dn"):
        loads[name].wait()
    npre[...] = dot(own[...], w_pn[pl.ds(0, m), :]) + vec[2]
    scatter_rows(gtab_r, 0, g, dot(gnodes[...], w_de[pl.ds(m, m), :]) + vec[4])
    for start in range(0, gedge_count, GRID_BLOCK):
        rows = pl.ds(start, GRID_BLOCK)
        slot = gpicked.at[start // GRID_BLOCK % 2]
        pick(slot, gtab_r, greceivers, start, GRID_BLOCK)
        gpre[rows, :] = dot(gedges[rows, :], w_de[pl.ds(2 * m, m), :]) + gathered_rows(slot, 0, GRID_BLOCK)
    gnpre[...] = dot(gnodes[...], w_dn[pl.ds(0, m), :]) + vec[6]

    for name in ("recv_row", "grecv_row", "w_po", "w_pno", "w_do", "w_dno"):
        loads[name].wait()

    direct = everyone.at[pl.ds(0, (half - 1) * offer)]
    pltpu.make_async_copy(direct, direct, recv_sem).wait()

    def forward(step, carry):
        region = lax.rem(me + 2 * step, regions)
        to_partner(block_of(region), region)
        return carry

    lax.fori_loop(1, half, forward, 0)
    passed = everyone.at[pl.ds(0, half * offer)]
    pltpu.make_async_copy(passed, passed, pass_recv_sem).wait()
    pltpu.make_async_copy(passed, passed, pass_send_sem).wait()
    pltpu.make_async_copy(direct, direct, send_sem).wait()
    wanted = dot(lane_hot(need_col, 0, regions * offer), everyone[...])
    scatter_rows(tab_s, n, slots, dot(wanted.astype(BF16), w_pe[pl.ds(0, m), :]))

    for start in range(0, edge_count, BLOCK):
        rows = pl.ds(start, BLOCK)
        slot = picked.at[start // BLOCK % 2]
        pick(slot, tab_s, senders, start, BLOCK)
        act = pre[rows, :] + gathered_rows(slot, 0, BLOCK)
        message = normed(silu(act).astype(BF16), w_po[...], vec[1]) + edges[rows, :].astype(F32)
        place = lax.broadcasted_iota(I32, (1, BLOCK), 1) + start
        targets = jnp.where(place < live[0], recv_row[:, start : start + BLOCK], -1)
        part = dot(row_hot(targets, n), message.astype(BF16))
        total[...] = part if start == 0 else total[...] + part

    act = npre[...] + dot(total[...].astype(BF16), w_pn[pl.ds(m, m), :])
    updated[...] = (
        own[...].astype(F32) + normed(silu(act).astype(BF16), w_pno[...], vec[3])
    ).astype(BF16)
    pub_out[...] = dot(offer_hot, updated[...]).astype(BF16)
    copies = []
    for slot, offset in enumerate(OFFSETS):
        copy = pltpu.make_async_remote_copy(
            src_ref=pub_out,
            dst_ref=arrived.at[pl.ds(slot * offer, offer)],
            send_sem=out_send_sem.at[slot],
            recv_sem=out_recv_sem.at[slot],
            device_id={"region": lax.rem(me - offset + regions, regions)},
            device_id_type=pl.DeviceIdType.MESH,
        )
        copy.start()
        copies.append(copy)
    writing = pltpu.make_async_copy(updated, mesh_out_ref, write_sem.at[0])
    writing.start()
    scatter_rows(gtab_s, 0, n, dot(updated[...], w_de[pl.ds(0, m), :]))
    for copy in copies:
        copy.wait()
    wanted = dot(lane_hot(gneed_col, 0, arrived.shape[0]), arrived[...])
    scatter_rows(gtab_s, n, gslots, dot(wanted.astype(BF16), w_de[pl.ds(0, m), :]))

    for start in range(0, gedge_count, GRID_BLOCK):
        rows = pl.ds(start, GRID_BLOCK)
        slot = gpicked.at[start // GRID_BLOCK % 2]
        pick(slot, gtab_s, gsenders, start, GRID_BLOCK)
        act = gpre[rows, :] + gathered_rows(slot, 0, GRID_BLOCK)
        message = normed(silu(act).astype(BF16), w_do[...], vec[5]) + gedges[rows, :].astype(F32)
        part = dot(row_hot(grecv_row[:, start : start + GRID_BLOCK], g), message.astype(BF16))
        gtotal[...] = part if start == 0 else gtotal[...] + part

    act = gnpre[...] + dot(gtotal[...].astype(BF16), w_dn[pl.ds(m, m), :])
    grid_stage[...] = (
        gnodes[...].astype(F32) + normed(silu(act).astype(BF16), w_dno[...], vec[7])
    ).astype(BF16)
    gwriting = pltpu.make_async_copy(grid_stage, grid_out_ref, write_sem.at[1])
    gwriting.start()
    writing.wait()
    gwriting.wait()


def local(
    mesh_nodes, mesh_edges, grid_nodes, grid_edges,
    boundary, mesh_need, mesh_sender, mesh_receiver, mesh_live,
    grid_need, grid_sender, grid_receiver,
    *weights,
):
    regions = mesh_need.shape[1]
    pair = mesh_need.shape[2]
    offer = boundary.shape[1]
    n, m = mesh_nodes.shape
    g = grid_nodes.shape[0]
    edge_count = mesh_edges.shape[0]
    gedge_count = grid_edges.shape[0]
    slots = regions * pair
    gslots = len(OFFSETS) * pair
    chunks = m // LANES
    weights = [w if w.ndim == 2 else w.reshape(1, -1) for w in weights]

    sizes = (regions, offer, pair, n, m, edge_count, g, gedge_count)
    v = pltpu.VMEM
    s = pltpu.SMEM
    dma = pltpu.SemaphoreType.DMA
    scratch = [
        s((1,), I32), s((1, offer), I32), s((pair, regions), I32), s((len(OFFSETS), pair), I32),
        s((1, edge_count), I32), s((1, edge_count), I32), s((1, gedge_count), I32), s((1, gedge_count), I32),
        v((n, m), BF16), v((edge_count, m), BF16), v((g, m), BF16), v((gedge_count, m), BF16),
        v((1, edge_count), I32), v((1, gedge_count), I32),
        v((3 * m, m), BF16), v((m, m), BF16), v((2 * m, m), BF16), v((m, m), BF16),
        v((3 * m, m), BF16), v((m, m), BF16), v((2 * m, m), BF16), v((m, m), BF16),
        v((8, 1, m), F32),
        v(((n + slots) * chunks, LANES), F32), v((n * chunks, LANES), F32),
        v(((n + gslots) * chunks, LANES), F32), v((g * chunks, LANES), F32),
        v((2, BLOCK * chunks, LANES), F32), v((2, GRID_BLOCK * chunks, LANES), F32),
        v((edge_count, m), F32), v((gedge_count, m), F32), v((n, m), F32), v((g, m), F32),
        v((n, m), F32), v((g, m), F32), v((n, m), BF16),
        v((offer, m), BF16), v((regions * offer, m), BF16), v((offer, m), BF16),
        v((len(OFFSETS) * offer, m), BF16), v((8, LANES), BF16), v((g, m), BF16),
        dma((2,)), dma((44,)),
        dma, dma, dma, dma,
        dma((len(OFFSETS),)), dma((len(OFFSETS),)),
    ]
    hbm = pl.BlockSpec(memory_space=pltpu.HBM)
    return pl.pallas_call(
        functools.partial(kernel, sizes),
        out_shape=(
            jax.ShapeDtypeStruct((n, m), BF16),
            jax.ShapeDtypeStruct((g, m), BF16),
        ),
        in_specs=[hbm] * 28,
        out_specs=(pl.BlockSpec(memory_space=pl.ANY),) * 2,
        scratch_shapes=scratch,
        compiler_params=pltpu.CompilerParams(
            collective_id=0, has_side_effects=True, vmem_limit_bytes=56 * 1024 * 1024
        ),
        name="layer",
    )(
        mesh_live, boundary, jnp.swapaxes(mesh_need[0], 0, 1), grid_need[0],
        mesh_nodes, mesh_edges, grid_nodes, grid_edges,
        mesh_sender, mesh_receiver, grid_sender, grid_receiver,
        *weights,
    )


def solution(mesh):
    both = P(("member", "region"), None)
    by = P("region", None)
    return jax.shard_map(
        local,
        mesh=mesh,
        in_specs=(
            both, by, both, by, by, P("region", None, None), by, by, P("region"),
            P("region", None, None), by, by,
        ) + (P(),) * 16,
        out_specs=(both, both),
        check_vma=False,
    )
```

```python
import functools

import jax
import jax.numpy as jnp
from jax import lax
from jax.experimental import pallas as pl
from jax.experimental.pallas import tpu as pltpu
from jax.sharding import PartitionSpec as P

F32 = jnp.float32
BF16 = jnp.bfloat16
I32 = jnp.int32
OFFSETS = (-2, -1, 1, 2)
LANES = 128
SUB = 8
BLOCK = 512
GRID_BLOCK = 384


def dot(a, b):
    return jnp.dot(a, b, preferred_element_type=F32)


def silu_of_half(half):
    half = half.astype(BF16)
    return half * jnp.tanh(half) + half


def normed(hidden, w_centred, gain):
    centred = dot(hidden, w_centred)
    spread = jnp.mean(centred * centred, axis=-1, keepdims=True)
    return centred * lax.rsqrt(spread + 0.25) * gain


def centre(w_ref):
    w = w_ref[...].astype(F32)
    w_ref[...] = (w - jnp.mean(w, axis=-1, keepdims=True)).astype(BF16)


def lane_hot(column, first, count):
    lane = lax.broadcasted_iota(I32, column.shape, 1) + first
    pieces = [
        jnp.where(column == lane + start, 1.0, 0.0).astype(BF16) for start in range(0, count, LANES)
    ]
    return pieces[0] if len(pieces) == 1 else jnp.concatenate(pieces, axis=1)


def row_mask(row, count):
    place = lax.broadcasted_iota(I32, (count, row.shape[1]), 0)
    return jnp.where(place == row, 1.0, 0.0)


def row_hot(row, count):
    return row_mask(row, count).astype(BF16)


def column_of(scalars):
    sub = lax.broadcasted_iota(I32, (SUB, LANES), 0)
    pieces = []
    for start in range(0, len(scalars), SUB):
        piece = jnp.full((SUB, LANES), scalars[start], I32)
        for k in range(1, SUB):
            piece = jnp.where(sub == k, scalars[start + k], piece)
        pieces.append(piece)
    return pieces[0] if len(pieces) == 1 else jnp.concatenate(pieces, axis=0)


def up(count, unit=LANES):
    return -(-count // unit) * unit


def kernel(
    sizes,
    live_hbm,
    boundary_hbm,
    need_hbm,
    gneed_hbm,
    mesh_nodes_hbm,
    mesh_edges_hbm,
    grid_nodes_hbm,
    grid_edges_hbm,
    mesh_sender_hbm,
    mesh_receiver_hbm,
    grid_sender_hbm,
    grid_receiver_hbm,
    pe_in, pe_b, pe_out, pe_g,
    pn_in, pn_b, pn_out, pn_g,
    de_in, de_b, de_out, de_g,
    dn_in, dn_b, dn_out, dn_g,
    updated, gtotal, gnpre, gnodes, w_dn, w_dno, vec,
    live, offers, need, gneed, senders, receivers, gsenders, greceivers,
    own, edges, gedges, recv_row, send_row, grecv_row, gsend_row, scaled_rows,
    w_pe, w_po, w_pn, w_pno, w_de, w_do,
    tab_s, tab_r, gtab_s, gtab_r, picked, gpicked,
    pre, gpre, npre, npre_offer, total, hot, ghot, rem,
    pub, everyone, pub_out, arrived,
    load_sem, index_sem, send_sem, pass_sem, recv_sem, out_send_sem, out_recv_sem,
):
    regions, offer, pair, n, m, edge_count, g, gedge_count = sizes
    slots, gslots = regions * pair, len(OFFSETS) * pair
    chunks = m // LANES
    me = lax.axis_index("region")

    loads = {}

    def load(name, source, target):
        copy = pltpu.make_async_copy(source, target, load_sem.at[len(loads)])
        copy.start()
        loads[name] = copy

    load("offers", boundary_hbm, offers)
    load("own", mesh_nodes_hbm, own)

    barrier = pltpu.get_barrier_semaphore()

    def greet(step, carry):
        pl.semaphore_signal(
            barrier,
            inc=1,
            device_id={"region": lax.rem(me + step, regions)},
            device_id_type=pl.DeviceIdType.MESH,
        )
        return carry

    lax.fori_loop(1, regions, greet, 0)

    load("w_s", pe_in.at[pl.ds(0, m)], w_pe.at[pl.ds(0, m)])
    load("w_r", pe_in.at[pl.ds(m, m)], w_pe.at[pl.ds(m, m)])
    for at, one in enumerate((pe_b, pe_g, pn_b, pn_g, de_b, de_g, dn_b, dn_g)):
        load(("vec", at), one, vec.at[at])
    load("recv_row", mesh_receiver_hbm, recv_row)
    load("send_row", mesh_sender_hbm, send_row)
    load("grecv_row", grid_receiver_hbm, grecv_row)
    load("gsend_row", grid_sender_hbm, gsend_row)
    load("need", need_hbm, need)
    load("gneed", gneed_hbm, gneed)
    load("live", live_hbm, live)
    load("w_e", pe_in.at[pl.ds(2 * m, m)], w_pe.at[pl.ds(2 * m, m)])
    for start in range(0, edge_count, BLOCK):
        load(("edges", start), mesh_edges_hbm.at[pl.ds(start, BLOCK)], edges.at[pl.ds(start, BLOCK)])
    load("w_pn", pn_in, w_pn)
    load("gnodes", grid_nodes_hbm, gnodes)
    load("w_de", de_in, w_de)
    load("w_po", pe_out, w_po)
    load("w_pno", pn_out, w_pno)
    load("w_dn", dn_in, w_dn)
    load("gedges", grid_edges_hbm, gedges)
    load("w_do", de_out, w_do)
    load("w_dno", dn_out, w_dno)

    loads["offers"].wait()
    offer_col = column_of([offers[0, k] for k in range(offer)])
    offer_hot = lane_hot(offer_col, 0, n)
    loads["own"].wait()
    pub[...] = dot(offer_hot, own[...]).astype(BF16)
    pl.semaphore_wait(barrier, regions - 1)

    chips, chip, core = regions // 2, me // 2, lax.rem(me, 2)

    rings = chips // 2
    ring, lane_y = chip // 2, lax.rem(chip, 2)
    hops = sorted(
        ((dz, dy) for dz in range(rings) for dy in range(2) if dz or dy),
        key=lambda hop: (-min(hop[0], rings - hop[0]) - hop[1], -hop[0], -hop[1]),
    )

    def chip_to(step):
        dz, dy = hops[step]
        return 2 * lax.rem(ring + dz, rings) + lax.rem(lane_y + dy, 2)

    def chip_from(step):
        dz, dy = hops[step]
        return 2 * lax.rem(ring - dz + rings, rings) + lax.rem(lane_y + dy, 2)

    def block_of(region):
        return everyone.at[pl.ds(pl.multiple_of(region * offer, offer), offer)]

    def push(source, region, target, sem):
        return pltpu.make_async_remote_copy(
            src_ref=source,
            dst_ref=block_of(region),
            send_sem=sem,
            recv_sem=recv_sem.at[region],
            device_id={"region": target},
            device_id_type=pl.DeviceIdType.MESH,
        )

    def came(region):
        block = block_of(region)
        pltpu.make_async_copy(block, block, recv_sem.at[region]).wait()

    def to_chip(step):
        return push(pub, me, 2 * chip_to(step) + core, send_sem.at[step])

    def to_partner(step):
        region = 2 * chip_from(step) + core
        return push(block_of(region), region, 2 * chip + 1 - core, pass_sem.at[step])

    own_to_partner = push(pub, me, 2 * chip + 1 - core, pass_sem.at[len(hops)])
    for step in range(len(hops)):
        to_chip(step).start()
    own_to_partner.start()
    everyone[pl.ds(pl.multiple_of(me * offer, offer), offer), :] = pub[...]

    def scatter_rows(target, first, rows, values):
        for c in range(chunks):
            target[pl.ds(first * chunks + c, rows, stride=chunks), :] = values[:, c * LANES : (c + 1) * LANES]

    def gathered_rows(source, first, rows):
        return jnp.concatenate(
            [source[pl.ds(first * chunks + c, rows, stride=chunks), :] for c in range(chunks)], axis=1
        )

    def pick(target, table, index, first, count, table_too=None, index_too=None):
        def one(at, carry):
            row = table[pl.ds(index[0, first + at], chunks), :]
            if table_too is not None:
                row = row + table_too[pl.ds(index_too[0, first + at], chunks), :]
            target[pl.ds(at * chunks, chunks), :] = row
            return carry

        lax.fori_loop(0, count, one, 0, unroll=True)

    scaled = []
    for at, (name, source, target) in enumerate((
        ("recv_row", recv_row, receivers), ("send_row", send_row, senders),
        ("grecv_row", grecv_row, greceivers), ("gsend_row", gsend_row, gsenders),
    )):
        loads[name].wait()
        width = source.shape[1]
        scaled_rows[at, :, pl.ds(0, width)] = jnp.minimum(source[...], n) * chunks
        copy = pltpu.make_async_copy(scaled_rows.at[at, :, pl.ds(0, width)], target, index_sem.at[at])
        copy.start()
        scaled.append(copy)
    for at in range(8):
        loads[("vec", at)].wait()
    loads["w_r"].wait()
    scatter_rows(tab_r, 0, n, dot(own[...], w_pe[pl.ds(m, m), :]) + vec[0])
    loads["w_s"].wait()
    scatter_rows(tab_s, 0, n, dot(own[...], w_pe[pl.ds(0, m), :]))
    tab_s[pl.ds(n * chunks, SUB), :] = jnp.zeros((SUB, LANES), F32)
    gtab_s[pl.ds(n * chunks, SUB), :] = jnp.zeros((SUB, LANES), F32)
    for name in ("need", "gneed", "live"):
        loads[name].wait()
    for copy in scaled:
        copy.wait()
    need_col = column_of([need[k, s] + s * offer for s in range(regions) for k in range(pair)])
    gneed_col = column_of([gneed[j, k] + j * offer for j in range(len(OFFSETS)) for k in range(pair)])
    gneed_hot = lane_hot(gneed_col, 0, arrived.shape[0])
    loads["w_e"].wait()
    for start in range(0, edge_count, BLOCK):
        loads[("edges", start)].wait()
    for start in range(0, edge_count, BLOCK):
        rows = pl.ds(start, BLOCK)
        slot = picked.at[start // BLOCK % 2]
        pick(slot, tab_r, receivers, start, BLOCK, tab_s, senders)
        pre[rows, :] = 0.5 * (dot(edges[rows, :], w_pe[pl.ds(2 * m, m), :]) + gathered_rows(slot, 0, BLOCK))
        remote = row_mask(send_row[:, start : start + BLOCK] - n, up(slots))
        hot[rows, :] = jnp.transpose(remote)[:, :slots].astype(BF16)

    loads["gnodes"].wait()
    loads["w_de"].wait()
    scatter_rows(gtab_r, 0, g, dot(gnodes[...], w_de[pl.ds(m, m), :]) + vec[4])
    for start in range(0, gedge_count, GRID_BLOCK):
        remote = row_hot(gsend_row[:, start : start + GRID_BLOCK] - n, gslots)
        ghot[pl.ds(start, GRID_BLOCK), :] = lax.dot_general(
            remote, gneed_hot, (((0,), (0,)), ((), ())), preferred_element_type=F32
        ).astype(BF16)

    for step in range(len(hops)):
        came(2 * chip_from(step) + core)
        to_partner(step).start()
    for name in ("w_pn", "w_dn"):
        loads[name].wait()
    for name, w_out in (("w_po", w_po), ("w_pno", w_pno)):
        loads[name].wait()
        centre(w_out)
    w_pn[pl.ds(m, m), :] = w_pn[pl.ds(m, m), :] * 0.5
    w_dn[pl.ds(m, m), :] = w_dn[pl.ds(m, m), :] * 0.5
    npre[...] = 0.5 * (dot(own[...], w_pn[pl.ds(0, m), :]) + vec[2])
    npre_offer[...] = 0.5 * (dot(pub[...], w_pn[pl.ds(0, m), :]) + vec[2])
    gnpre[...] = 0.5 * (dot(gnodes[...], w_dn[pl.ds(0, m), :]) + vec[6])
    came(2 * chip + 1 - core)
    for step in range(len(hops)):
        came(2 * chip_from(step) + 1 - core)
    wanted = dot(lane_hot(need_col, 0, regions * offer), everyone[...])
    rem[...] = (0.5 * dot(wanted.astype(BF16), w_pe[pl.ds(0, m), :])).astype(BF16)

    for start in range(0, edge_count, BLOCK):
        rows = pl.ds(start, BLOCK)
        act = pre[rows, :] + dot(hot[rows, :], rem[...])
        message = normed(silu_of_half(act), w_po[...], vec[1]).astype(BF16) + edges[rows, :]
        place = lax.broadcasted_iota(I32, (1, BLOCK), 1) + start
        targets = jnp.where(place < live[0, 0], recv_row[:, start : start + BLOCK], -1)
        part = dot(row_hot(targets, n), message)
        total[...] = part if start == 0 else total[...] + part

    summed = total[...].astype(BF16)
    act = npre_offer[...] + dot(dot(offer_hot, summed).astype(BF16), w_pn[pl.ds(m, m), :])
    pub_out[...] = (pub[...].astype(F32) + normed(silu_of_half(act), w_pno[...], vec[3])).astype(BF16)
    copies = []
    for slot, offset in enumerate(OFFSETS):
        copy = pltpu.make_async_remote_copy(
            src_ref=pub_out,
            dst_ref=arrived.at[pl.ds(slot * offer, offer)],
            send_sem=out_send_sem.at[slot],
            recv_sem=out_recv_sem.at[slot],
            device_id={"region": lax.rem(me - offset + regions, regions)},
            device_id_type=pl.DeviceIdType.MESH,
        )
        copy.start()
        copies.append(copy)
    for name in ("gedges", "w_do", "w_dno"):
        loads[name].wait()
    act = npre[...] + dot(summed, w_pn[pl.ds(m, m), :])
    updated[...] = (own[...].astype(F32) + normed(silu_of_half(act), w_pno[...], vec[3])).astype(BF16)
    scatter_rows(gtab_s, 0, n, dot(updated[...], w_de[pl.ds(0, m), :]))
    for start in range(0, gedge_count, GRID_BLOCK):
        rows = pl.ds(start, GRID_BLOCK)
        slot = gpicked.at[start // GRID_BLOCK % 2]
        pick(slot, gtab_r, greceivers, start, GRID_BLOCK, gtab_s, gsenders)
        gpre[rows, :] = 0.5 * (dot(gedges[rows, :], w_de[pl.ds(2 * m, m), :]) + gathered_rows(slot, 0, GRID_BLOCK))
    centre(w_do)
    centre(w_dno)
    own_to_partner.wait_send()
    for step in range(len(hops)):
        to_chip(step).wait_send()
        to_partner(step).wait_send()
    for copy in copies:
        copy.wait()
    grem = (0.5 * dot(arrived[...], w_de[pl.ds(0, m), :])).astype(BF16)

    for start in range(0, gedge_count, GRID_BLOCK):
        rows = pl.ds(start, GRID_BLOCK)
        act = gpre[rows, :] + dot(ghot[rows, :], grem)
        message = normed(silu_of_half(act), w_do[...], vec[5]).astype(BF16) + gedges[rows, :]
        part = dot(row_hot(grecv_row[:, start : start + GRID_BLOCK], g), message)
        gtotal[...] = part if start == 0 else gtotal[...] + part


def finale(updated, gtotal, gnpre, gnodes, w_dn, w_dno, vec, mesh_out, grid_out, stage, sem):
    first = pltpu.make_async_copy(updated, mesh_out, sem.at[0])
    first.start()
    m = stage.shape[1]
    act = gnpre[...] + dot(gtotal[...].astype(BF16), w_dn[pl.ds(m, m), :])
    stage[...] = (
        gnodes[...].astype(F32) + normed(silu_of_half(act), w_dno[...], vec[7])
    ).astype(BF16)
    second = pltpu.make_async_copy(stage, grid_out, sem.at[1])
    second.start()
    first.wait()
    second.wait()


def local(
    mesh_nodes, mesh_edges, grid_nodes, grid_edges,
    boundary, mesh_need, mesh_sender, mesh_receiver, mesh_live,
    grid_need, grid_sender, grid_receiver,
    *weights,
):
    regions = mesh_need.shape[1]
    pair = mesh_need.shape[2]
    offer = boundary.shape[1]
    n, m = mesh_nodes.shape
    g = grid_nodes.shape[0]
    edge_count = mesh_edges.shape[0]
    gedge_count = grid_edges.shape[0]
    slots = regions * pair
    gslots = len(OFFSETS) * pair
    chunks = m // LANES
    weights = [w if w.ndim == 2 else w.reshape(1, -1) for w in weights]

    sizes = (regions, offer, pair, n, m, edge_count, g, gedge_count)
    v = pltpu.VMEM
    s = pltpu.SMEM
    dma = pltpu.SemaphoreType.DMA
    scratch = [
        s((1, 1), I32), s((1, offer), I32), s((pair, regions), I32), s((len(OFFSETS), pair), I32),
        s((1, edge_count), I32), s((1, edge_count), I32), s((1, gedge_count), I32), s((1, gedge_count), I32),
        v((n, m), BF16), v((edge_count, m), BF16), v((gedge_count, m), BF16),
        v((1, edge_count), I32), v((1, edge_count), I32), v((1, gedge_count), I32), v((1, gedge_count), I32),
        v((4, 1, edge_count), I32),
        v((3 * m, m), BF16), v((m, m), BF16), v((2 * m, m), BF16), v((m, m), BF16),
        v((3 * m, m), BF16), v((m, m), BF16),
        v((n * chunks + SUB, LANES), F32), v((n * chunks, LANES), F32),
        v((n * chunks + SUB, LANES), F32), v((g * chunks, LANES), F32),
        v((2, BLOCK * chunks, LANES), F32), v((2, GRID_BLOCK * chunks, LANES), F32),
        v((edge_count, m), F32), v((gedge_count, m), F32), v((n, m), F32), v((offer, m), F32),
        v((n, m), F32),
        v((edge_count, slots), BF16), v((gedge_count, len(OFFSETS) * offer), BF16), v((slots, m), BF16),
        v((offer, m), BF16), v((regions * offer, m), BF16), v((offer, m), BF16),
        v((len(OFFSETS) * offer, m), BF16),
        dma((44,)), dma((4,)), dma((regions // 2,)), dma((regions // 2,)), dma((regions,)),
        dma((len(OFFSETS),)), dma((len(OFFSETS),)),
    ]
    hbm = pl.BlockSpec(memory_space=pltpu.HBM)
    handed = pl.pallas_call(
        functools.partial(kernel, sizes),
        out_shape=(
            v((n, m), BF16), v((g, m), F32), v((g, m), F32), v((g, m), BF16),
            v((2 * m, m), BF16), v((m, m), BF16), v((8, 1, m), F32),
        ),
        in_specs=[hbm] * 28,
        out_specs=(pl.BlockSpec(memory_space=pltpu.VMEM),) * 7,
        scratch_shapes=scratch,
        compiler_params=pltpu.CompilerParams(
            collective_id=0, has_side_effects=True, vmem_limit_bytes=56 * 1024 * 1024
        ),
        name="layer",
    )(
        mesh_live.reshape(1, 1), boundary, jnp.swapaxes(mesh_need[0], 0, 1), grid_need[0],
        mesh_nodes, mesh_edges, grid_nodes, grid_edges,
        mesh_sender, mesh_receiver, grid_sender, grid_receiver,
        *weights,
    )
    return pl.pallas_call(
        finale,
        out_shape=(jax.ShapeDtypeStruct((n, m), BF16), jax.ShapeDtypeStruct((g, m), BF16)),
        in_specs=[pl.BlockSpec(memory_space=pltpu.VMEM)] * 7,
        out_specs=(pl.BlockSpec(memory_space=pl.ANY),) * 2,
        scratch_shapes=[v((g, m), BF16), dma((2,))],
        compiler_params=pltpu.CompilerParams(vmem_limit_bytes=16 * 1024 * 1024),
        name="finale",
    )(*(pltpu.with_memory_space_constraint(one, pltpu.VMEM) for one in handed))


def solution(mesh):
    both = P(("member", "region"), None)
    by = P("region", None)
    return jax.shard_map(
        local,
        mesh=mesh,
        in_specs=(
            both, by, both, by, by, P("region", None, None), by, by, P("region"),
            P("region", None, None), by, by,
        ) + (P(),) * 16,
        out_specs=(both, both),
        check_vma=False,
    )
```

```python
import functools

import jax
import jax.numpy as jnp
from jax import lax
from jax.experimental import pallas as pl
from jax.experimental.pallas import tpu as pltpu
from jax.sharding import PartitionSpec as P

F32 = jnp.float32
BF16 = jnp.bfloat16
I32 = jnp.int32
OFFSETS = (-2, -1, 1, 2)
LANES = 128
SUB = 8
BLOCK = 1024
GRID_BLOCK = 384


def dot(a, b):
    return jnp.dot(a, b, preferred_element_type=F32)


def silu_of_half(half):
    half = half.astype(BF16)
    return half * jnp.tanh(half) + half


def normed(hidden, w_centred, gain):
    centred = dot(hidden, w_centred)
    spread = jnp.mean(centred * centred, axis=-1, keepdims=True)
    return centred * lax.rsqrt(spread + 0.25) * gain


def centre(w_ref):
    w = w_ref[...].astype(F32)
    w_ref[...] = (w - jnp.mean(w, axis=-1, keepdims=True)).astype(BF16)


def lane_hot(column, first, count):
    lane = lax.broadcasted_iota(I32, column.shape, 1) + first
    pieces = [
        jnp.where(column == lane + start, 1.0, 0.0).astype(BF16) for start in range(0, count, LANES)
    ]
    return pieces[0] if len(pieces) == 1 else jnp.concatenate(pieces, axis=1)


def row_mask(row, count):
    place = lax.broadcasted_iota(I32, (count, row.shape[1]), 0)
    return jnp.where(place == row, 1.0, 0.0)


def row_hot(row, count):
    return row_mask(row, count).astype(BF16)


def column_of(scalars):
    sub = lax.broadcasted_iota(I32, (SUB, LANES), 0)
    pieces = []
    for start in range(0, len(scalars), SUB):
        piece = jnp.full((SUB, LANES), scalars[start], I32)
        for k in range(1, SUB):
            piece = jnp.where(sub == k, scalars[start + k], piece)
        pieces.append(piece)
    return pieces[0] if len(pieces) == 1 else jnp.concatenate(pieces, axis=0)


def up(count, unit=LANES):
    return -(-count // unit) * unit


def kernel(
    sizes,
    live_hbm,
    boundary_hbm,
    need_hbm,
    gneed_hbm,
    mesh_nodes_hbm,
    mesh_edges_hbm,
    grid_nodes_hbm,
    grid_edges_hbm,
    mesh_sender_hbm,
    mesh_receiver_hbm,
    grid_sender_hbm,
    grid_receiver_hbm,
    pe_in, pe_b, pe_out, pe_g,
    pn_in, pn_b, pn_out, pn_g,
    de_in, de_b, de_out, de_g,
    dn_in, dn_b, dn_out, dn_g,
    updated, gtotal, gnpre, gnodes, w_dn, w_dno, vec,
    live, offers, need, gneed, senders, receivers, gsenders, greceivers,
    own, edges, gedges, recv_row, send_row, grecv_row, gsend_row, scaled_rows,
    w_pe, w_po, w_pn, w_pno, w_de, w_do,
    tab_s, tab_r, gtab_s, gtab_r, picked, gpicked,
    pre, gpre, npre, npre_offer, total, hot, ghot, rem,
    pub, everyone, pub_out, arrived,
    load_sem, index_sem, send_sem, pass_sem, recv_sem, out_send_sem, out_recv_sem,
):
    regions, offer, pair, n, m, edge_count, g, gedge_count = sizes
    slots, gslots = regions * pair, len(OFFSETS) * pair
    chunks = m // LANES
    me = lax.axis_index("region")

    loads = {}

    def load(name, source, target):
        copy = pltpu.make_async_copy(source, target, load_sem.at[len(loads)])
        copy.start()
        loads[name] = copy

    load("offers", boundary_hbm, offers)
    load("own", mesh_nodes_hbm, own)

    barrier = pltpu.get_barrier_semaphore()

    def greet(step, carry):
        pl.semaphore_signal(
            barrier,
            inc=1,
            device_id={"region": lax.rem(me + step, regions)},
            device_id_type=pl.DeviceIdType.MESH,
        )
        return carry

    lax.fori_loop(1, regions, greet, 0)

    load("w_s", pe_in.at[pl.ds(0, m)], w_pe.at[pl.ds(0, m)])
    load("w_r", pe_in.at[pl.ds(m, m)], w_pe.at[pl.ds(m, m)])
    for at, one in enumerate((pe_b, pe_g, pn_b, pn_g, de_b, de_g, dn_b, dn_g)):
        load(("vec", at), one, vec.at[at])
    load("recv_row", mesh_receiver_hbm, recv_row)
    load("send_row", mesh_sender_hbm, send_row)
    load("grecv_row", grid_receiver_hbm, grecv_row)
    load("gsend_row", grid_sender_hbm, gsend_row)
    load("need", need_hbm, need)
    load("gneed", gneed_hbm, gneed)
    load("live", live_hbm, live)
    load("w_e", pe_in.at[pl.ds(2 * m, m)], w_pe.at[pl.ds(2 * m, m)])
    for start in range(0, edge_count, BLOCK):
        load(("edges", start), mesh_edges_hbm.at[pl.ds(start, BLOCK)], edges.at[pl.ds(start, BLOCK)])
    load("w_pn", pn_in, w_pn)
    load("gnodes", grid_nodes_hbm, gnodes)
    load("w_de", de_in, w_de)
    load("w_po", pe_out, w_po)
    load("w_pno", pn_out, w_pno)
    load("w_dn", dn_in, w_dn)
    load("gedges", grid_edges_hbm, gedges)
    load("w_do", de_out, w_do)
    load("w_dno", dn_out, w_dno)

    loads["offers"].wait()
    offer_col = column_of([offers[0, k] for k in range(offer)])
    offer_hot = lane_hot(offer_col, 0, n)
    loads["own"].wait()
    pub[...] = dot(offer_hot, own[...]).astype(BF16)
    pl.semaphore_wait(barrier, regions - 1)

    chips, chip, core = regions // 2, me // 2, lax.rem(me, 2)

    rings = chips // 2
    ring, lane_y = chip // 2, lax.rem(chip, 2)
    hops = sorted(
        ((dz, dy) for dz in range(rings) for dy in range(2) if dz or dy),
        key=lambda hop: (-min(hop[0], rings - hop[0]) - hop[1], -hop[0], -hop[1]),
    )

    def chip_to(step):
        dz, dy = hops[step]
        return 2 * lax.rem(ring + dz, rings) + lax.rem(lane_y + dy, 2)

    def chip_from(step):
        dz, dy = hops[step]
        return 2 * lax.rem(ring - dz + rings, rings) + lax.rem(lane_y + dy, 2)

    def block_of(region):
        return everyone.at[pl.ds(pl.multiple_of(region * offer, offer), offer)]

    def push(source, region, target, sem):
        return pltpu.make_async_remote_copy(
            src_ref=source,
            dst_ref=block_of(region),
            send_sem=sem,
            recv_sem=recv_sem.at[region],
            device_id={"region": target},
            device_id_type=pl.DeviceIdType.MESH,
        )

    def came(region):
        block = block_of(region)
        pltpu.make_async_copy(block, block, recv_sem.at[region]).wait()

    def to_chip(step):
        return push(pub, me, 2 * chip_to(step) + core, send_sem.at[step])

    def to_partner(step):
        region = 2 * chip_from(step) + core
        return push(block_of(region), region, 2 * chip + 1 - core, pass_sem.at[step])

    own_to_partner = push(pub, me, 2 * chip + 1 - core, pass_sem.at[len(hops)])
    for step in range(len(hops)):
        to_chip(step).start()
    own_to_partner.start()
    everyone[pl.ds(pl.multiple_of(me * offer, offer), offer), :] = pub[...]

    def scatter_rows(target, first, rows, values):
        for c in range(chunks):
            target[pl.ds(first * chunks + c, rows, stride=chunks), :] = values[:, c * LANES : (c + 1) * LANES]

    def gathered_rows(source, first, rows):
        return jnp.concatenate(
            [source[pl.ds(first * chunks + c, rows, stride=chunks), :] for c in range(chunks)], axis=1
        )

    def pick(target, table, index, first, count, table_too=None, index_too=None):
        def one(at, carry):
            row = table[pl.ds(index[0, first + at], chunks), :]
            if table_too is not None:
                row = row + table_too[pl.ds(index_too[0, first + at], chunks), :]
            target[pl.ds(at * chunks, chunks), :] = row
            return carry

        lax.fori_loop(0, count, one, 0, unroll=True)

    scaled = []
    for at, (name, source, target) in enumerate((
        ("recv_row", recv_row, receivers), ("send_row", send_row, senders),
        ("grecv_row", grecv_row, greceivers), ("gsend_row", gsend_row, gsenders),
    )):
        loads[name].wait()
        width = source.shape[1]
        scaled_rows[at, :, pl.ds(0, width)] = jnp.minimum(source[...], n) * chunks
        copy = pltpu.make_async_copy(scaled_rows.at[at, :, pl.ds(0, width)], target, index_sem.at[at])
        copy.start()
        scaled.append(copy)
    for at in range(8):
        loads[("vec", at)].wait()
    loads["w_r"].wait()
    scatter_rows(tab_r, 0, n, dot(own[...], w_pe[pl.ds(m, m), :]) + vec[0])
    loads["w_s"].wait()
    scatter_rows(tab_s, 0, n, dot(own[...], w_pe[pl.ds(0, m), :]))
    tab_s[pl.ds(n * chunks, SUB), :] = jnp.zeros((SUB, LANES), F32)
    gtab_s[pl.ds(n * chunks, SUB), :] = jnp.zeros((SUB, LANES), F32)
    for name in ("need", "gneed", "live"):
        loads[name].wait()
    for copy in scaled:
        copy.wait()
    need_col = column_of([need[k, s] + s * offer for s in range(regions) for k in range(pair)])
    gneed_col = column_of([gneed[j, k] + j * offer for j in range(len(OFFSETS)) for k in range(pair)])
    gneed_hot = lane_hot(gneed_col, 0, arrived.shape[0])
    loads["w_e"].wait()
    for start in range(0, edge_count, BLOCK):
        loads[("edges", start)].wait()
    for start in range(0, edge_count, BLOCK):
        rows = pl.ds(start, BLOCK)
        slot = picked.at[start // BLOCK % 2]
        pick(slot, tab_r, receivers, start, BLOCK, tab_s, senders)
        pre[rows, :] = 0.5 * (dot(edges[rows, :], w_pe[pl.ds(2 * m, m), :]) + gathered_rows(slot, 0, BLOCK))
        remote = row_mask(send_row[:, start : start + BLOCK] - n, up(slots))
        hot[rows, :] = jnp.transpose(remote)[:, :slots].astype(BF16)

    loads["gnodes"].wait()
    loads["w_de"].wait()
    scatter_rows(gtab_r, 0, g, dot(gnodes[...], w_de[pl.ds(m, m), :]) + vec[4])
    for start in range(0, gedge_count, GRID_BLOCK):
        remote = row_hot(gsend_row[:, start : start + GRID_BLOCK] - n, gslots)
        ghot[pl.ds(start, GRID_BLOCK), :] = lax.dot_general(
            remote, gneed_hot, (((0,), (0,)), ((), ())), preferred_element_type=F32
        ).astype(BF16)

    for step in range(len(hops)):
        came(2 * chip_from(step) + core)
        to_partner(step).start()
    for name in ("w_pn", "w_dn"):
        loads[name].wait()
    for name, w_out in (("w_po", w_po), ("w_pno", w_pno)):
        loads[name].wait()
        centre(w_out)
    w_pn[pl.ds(m, m), :] = w_pn[pl.ds(m, m), :] * 0.5
    w_dn[pl.ds(m, m), :] = w_dn[pl.ds(m, m), :] * 0.5
    npre[...] = 0.5 * (dot(own[...], w_pn[pl.ds(0, m), :]) + vec[2])
    npre_offer[...] = 0.5 * (dot(pub[...], w_pn[pl.ds(0, m), :]) + vec[2])
    gnpre[...] = 0.5 * (dot(gnodes[...], w_dn[pl.ds(0, m), :]) + vec[6])
    came(2 * chip + 1 - core)
    for step in range(len(hops)):
        came(2 * chip_from(step) + 1 - core)
    wanted = dot(lane_hot(need_col, 0, regions * offer), everyone[...])
    rem[...] = (0.5 * dot(wanted.astype(BF16), w_pe[pl.ds(0, m), :])).astype(BF16)

    for start in range(0, edge_count, BLOCK):
        rows = pl.ds(start, BLOCK)
        act = pre[rows, :] + dot(hot[rows, :], rem[...])
        message = normed(silu_of_half(act), w_po[...], vec[1]).astype(BF16) + edges[rows, :]
        place = lax.broadcasted_iota(I32, (1, BLOCK), 1) + start
        targets = jnp.where(place < live[0, 0], recv_row[:, start : start + BLOCK], -1)
        part = dot(row_hot(targets, n), message)
        total[...] = part if start == 0 else total[...] + part

    summed = total[...].astype(BF16)
    act = npre_offer[...] + dot(dot(offer_hot, summed).astype(BF16), w_pn[pl.ds(m, m), :])
    pub_out[...] = (pub[...].astype(F32) + normed(silu_of_half(act), w_pno[...], vec[3])).astype(BF16)
    copies = []
    for slot, offset in enumerate(OFFSETS):
        copy = pltpu.make_async_remote_copy(
            src_ref=pub_out,
            dst_ref=arrived.at[pl.ds(slot * offer, offer)],
            send_sem=out_send_sem.at[slot],
            recv_sem=out_recv_sem.at[slot],
            device_id={"region": lax.rem(me - offset + regions, regions)},
            device_id_type=pl.DeviceIdType.MESH,
        )
        copy.start()
        copies.append(copy)
    for name in ("gedges", "w_do", "w_dno"):
        loads[name].wait()
    act = npre[...] + dot(summed, w_pn[pl.ds(m, m), :])
    updated[...] = (own[...].astype(F32) + normed(silu_of_half(act), w_pno[...], vec[3])).astype(BF16)
    scatter_rows(gtab_s, 0, n, dot(updated[...], w_de[pl.ds(0, m), :]))
    for start in range(0, gedge_count, GRID_BLOCK):
        rows = pl.ds(start, GRID_BLOCK)
        slot = gpicked.at[start // GRID_BLOCK % 2]
        pick(slot, gtab_r, greceivers, start, GRID_BLOCK, gtab_s, gsenders)
        gpre[rows, :] = 0.5 * (dot(gedges[rows, :], w_de[pl.ds(2 * m, m), :]) + gathered_rows(slot, 0, GRID_BLOCK))
    centre(w_do)
    centre(w_dno)
    own_to_partner.wait_send()
    for step in range(len(hops)):
        to_chip(step).wait_send()
        to_partner(step).wait_send()
    for copy in copies:
        copy.wait()
    grem = (0.5 * dot(arrived[...], w_de[pl.ds(0, m), :])).astype(BF16)

    act = gpre[...] + dot(ghot[...], grem)
    message = normed(silu_of_half(act), w_do[...], vec[5]).astype(BF16) + gedges[...]
    gtotal[...] = dot(row_hot(grecv_row[...], g), message)


def finale(updated, gtotal, gnpre, gnodes, w_dn, w_dno, vec, mesh_out, grid_out, stage, sem):
    first = pltpu.make_async_copy(updated, mesh_out, sem.at[0])
    first.start()
    m = stage.shape[1]
    act = gnpre[...] + dot(gtotal[...].astype(BF16), w_dn[pl.ds(m, m), :])
    stage[...] = (
        gnodes[...].astype(F32) + normed(silu_of_half(act), w_dno[...], vec[7])
    ).astype(BF16)
    second = pltpu.make_async_copy(stage, grid_out, sem.at[1])
    second.start()
    first.wait()
    second.wait()


def local(
    mesh_nodes, mesh_edges, grid_nodes, grid_edges,
    boundary, mesh_need, mesh_sender, mesh_receiver, mesh_live,
    grid_need, grid_sender, grid_receiver,
    *weights,
):
    regions = mesh_need.shape[1]
    pair = mesh_need.shape[2]
    offer = boundary.shape[1]
    n, m = mesh_nodes.shape
    g = grid_nodes.shape[0]
    edge_count = mesh_edges.shape[0]
    gedge_count = grid_edges.shape[0]
    slots = regions * pair
    gslots = len(OFFSETS) * pair
    chunks = m // LANES
    weights = [w if w.ndim == 2 else w.reshape(1, -1) for w in weights]

    sizes = (regions, offer, pair, n, m, edge_count, g, gedge_count)
    v = pltpu.VMEM
    s = pltpu.SMEM
    dma = pltpu.SemaphoreType.DMA
    scratch = [
        s((1, 1), I32), s((1, offer), I32), s((pair, regions), I32), s((len(OFFSETS), pair), I32),
        s((1, edge_count), I32), s((1, edge_count), I32), s((1, gedge_count), I32), s((1, gedge_count), I32),
        v((n, m), BF16), v((edge_count, m), BF16), v((gedge_count, m), BF16),
        v((1, edge_count), I32), v((1, edge_count), I32), v((1, gedge_count), I32), v((1, gedge_count), I32),
        v((4, 1, edge_count), I32),
        v((3 * m, m), BF16), v((m, m), BF16), v((2 * m, m), BF16), v((m, m), BF16),
        v((3 * m, m), BF16), v((m, m), BF16),
        v((n * chunks + SUB, LANES), F32), v((n * chunks, LANES), F32),
        v((n * chunks + SUB, LANES), F32), v((g * chunks, LANES), F32),
        v((2, BLOCK * chunks, LANES), F32), v((2, GRID_BLOCK * chunks, LANES), F32),
        v((edge_count, m), F32), v((gedge_count, m), F32), v((n, m), F32), v((offer, m), F32),
        v((n, m), F32),
        v((edge_count, slots), BF16), v((gedge_count, len(OFFSETS) * offer), BF16), v((slots, m), BF16),
        v((offer, m), BF16), v((regions * offer, m), BF16), v((offer, m), BF16),
        v((len(OFFSETS) * offer, m), BF16),
        dma((44,)), dma((4,)), dma((regions // 2,)), dma((regions // 2,)), dma((regions,)),
        dma((len(OFFSETS),)), dma((len(OFFSETS),)),
    ]
    hbm = pl.BlockSpec(memory_space=pltpu.HBM)
    handed = pl.pallas_call(
        functools.partial(kernel, sizes),
        out_shape=(
            v((n, m), BF16), v((g, m), F32), v((g, m), F32), v((g, m), BF16),
            v((2 * m, m), BF16), v((m, m), BF16), v((8, 1, m), F32),
        ),
        in_specs=[hbm] * 28,
        out_specs=(pl.BlockSpec(memory_space=pltpu.VMEM),) * 7,
        scratch_shapes=scratch,
        compiler_params=pltpu.CompilerParams(
            collective_id=0, has_side_effects=True, vmem_limit_bytes=56 * 1024 * 1024
        ),
        name="layer",
    )(
        mesh_live.reshape(1, 1), boundary, jnp.swapaxes(mesh_need[0], 0, 1), grid_need[0],
        mesh_nodes, mesh_edges, grid_nodes, grid_edges,
        mesh_sender, mesh_receiver, grid_sender, grid_receiver,
        *weights,
    )
    return pl.pallas_call(
        finale,
        out_shape=(jax.ShapeDtypeStruct((n, m), BF16), jax.ShapeDtypeStruct((g, m), BF16)),
        in_specs=[pl.BlockSpec(memory_space=pltpu.VMEM)] * 7,
        out_specs=(pl.BlockSpec(memory_space=pl.ANY),) * 2,
        scratch_shapes=[v((g, m), BF16), dma((2,))],
        compiler_params=pltpu.CompilerParams(vmem_limit_bytes=16 * 1024 * 1024),
        name="finale",
    )(*(pltpu.with_memory_space_constraint(one, pltpu.VMEM) for one in handed))


def solution(mesh):
    both = P(("member", "region"), None)
    by = P("region", None)
    return jax.shard_map(
        local,
        mesh=mesh,
        in_specs=(
            both, by, both, by, by, P("region", None, None), by, by, P("region"),
            P("region", None, None), by, by,
        ) + (P(),) * 16,
        out_specs=(both, both),
        check_vma=False,
    )
```
